512 devices in a mesh: dp: 32 (over y, x), mp: 16 (over z, core).
Axes of the slice: x: 4, y: 8, z: 8, core: 2. Of those that a mesh axis runs over, the one named last changes fastest.
Arguments:
- buffer: bfloat16 [1048576, 256], P(('dp', 'mp')), may hold values from -24 to 24, as said below
- owner: int32 [524288, 1], P(('dp', 'mp')), may hold values from 0 to 511; in each aligned block of 1024 rows (0 to 1023, 1024 to 2047, ...) at most 8 rows name the same one
- local_row: int32 [524288], P(('dp', 'mp')), may hold values from 0 to 2047
- q_in: bfloat16 [2, 130, 256], replicated, may hold values from -0.5 to 0.5
- q_mid: bfloat16 [2, 256, 256], replicated, may hold values from -0.5 to 0.5
- q_out: bfloat16 [2, 256], replicated, may hold values from -0.5 to 0.5
- v_in: bfloat16 [124, 256], replicated, may hold values from -0.5 to 0.5
- v_mid: bfloat16 [256, 256], replicated, may hold values from -0.5 to 0.5
- v_out: bfloat16 [256], replicated, may hold values from -0.5 to 0.5
Outputs:
- q_values: float32 [2, 524288], P(None, ('dp', 'mp'))
- values: float32 [2, 524288], P(None, ('dp', 'mp'))
- targets: float32 [524288], P(('dp', 'mp'))
- q_loss: float32 [524288], P(('dp', 'mp'))
- value_loss: float32 [524288], P(('dp', 'mp'))
The draws below stay inside these ranges and needn't reach their ends.
Inputs may be any that keep to these rules, and one draw needn't show every extreme that they name: Owner o is the replay owner at position o of the devices in dp+mp order. In the rows of one reader no owner is named more than 8 times, a bound that some block reaches. `buffer`: action values lie in -1 to 1 and discounts in 0 to 0.99.
All inputs are finite; a program needn't handle non-finite values.
Results may differ from the reference program's by a relative error of at most 0.005.
Values may be sent and summed in bfloat16 or wider, within the bound.
No kernel may reach another device: no remote copies, remote signals or barrier semaphores. Data moves between devices by JAX's collectives and lax.ppermute only.
A program may use at most 64 MiB of HBM per device.

```python
import math
import jax
import jax.numpy as jnp
import numpy as np
from jax import lax

S = 124
A = 6
H = 256
ROWS_DEV = 2048
B_DEV = 1024
CAP = 8
ROWS = 1048576
BATCH = 524288
DEVICES = 512


def draw_buffer(key, part):
    keys = jax.random.split(jax.random.fold_in(key, 17), 5)
    states = jnp.clip(jax.random.normal(keys[0], (ROWS, S), jnp.float32), -6.0, 6.0)
    actions = jax.random.uniform(keys[1], (ROWS, A), jnp.float32, -1.0, 1.0)
    nexts = jnp.clip(jax.random.normal(keys[2], (ROWS, S), jnp.float32), -6.0, 6.0)
    reward = jnp.clip(jax.random.normal(keys[3], (ROWS, 1), jnp.float32), -6.0, 6.0)
    discount = jax.random.uniform(keys[4], (ROWS, 1), jnp.float32, 0.0, 0.99)
    return jnp.concatenate([states, actions, nexts, reward, discount], axis=1).astype(jnp.bfloat16)


def with_ends(result, key, low, largest):
    dims = result.shape
    place = [jax.random.randint(jax.random.fold_in(key, axis), (), 0, dims[axis]) for axis in range(len(dims))]
    result = result.at[tuple(place)].set(low)
    longest = dims.index(max(dims))
    place[longest] = (place[longest] + 1) % dims[longest]
    return result.at[tuple(place)].set(largest)


def assign_block(stream_key, own, number, rows, count, top, bound, skew):
    order = jax.random.permutation(stream_key, count)
    heavy_load, common = shares(count, rows * top, bound, skew, True), shares(count, rows * top, bound, skew, False)
    places = jnp.arange(count)

    def named(sizes, rotation):
        used = int((sizes > 0).sum())
        fixed = max(1, used // 4)
        moved = fixed + (places - fixed + rotation * (used - fixed)) % max(1, count - fixed)
        return jnp.zeros((count,), jnp.int32).at[order[jnp.where(places < fixed, places, moved)]].set(jnp.asarray(sizes, jnp.int32))

    sizes = jnp.where(number % 4 == 0, named(heavy_load, number // 4), named(common, number - number // 4 - 1))
    mixed = jax.random.permutation(jax.random.fold_in(own, 3), count)
    donor, taker = mixed[0:count // 2 * 2:2], mixed[1:count // 2 * 2:2]
    room = jnp.minimum(sizes[donor] - 1, bound - sizes[taker]) // 2
    room = jnp.where((donor == order[0]) | (taker == order[0]) | (sizes[taker] == 0), 0, jnp.maximum(room, 0))
    moved = jax.random.randint(jax.random.fold_in(own, 4), (count // 2,), 0, 1 << 20) % (room + 1)
    sizes = sizes.at[donor].add(-moved).at[taker].add(moved)
    members = jnp.searchsorted(jnp.cumsum(sizes), jnp.arange(rows * top), side="right").astype(jnp.int32)
    listing = members.reshape(top, rows).T
    listing = listing[jax.random.permutation(jax.random.fold_in(own, 1), rows)]
    rotation = jax.random.randint(jax.random.fold_in(own, 2), (rows, 1), 0, top)
    return jnp.take_along_axis(listing, (jnp.arange(top)[None, :] + rotation) % top, axis=1)


def shares(number_of, total, reach, skew, full):
    weights = [(1 << 20) // math.isqrt(grade ** skew) + 1 for grade in range(1, number_of + 1)]
    largest = reach if full else min(reach, max(-(-total // number_of), total * weights[0] // sum(weights)))
    least = 1 if total - largest >= number_of - 1 else 0
    holding, surplus = [largest] + [least] * (number_of - 1), total - largest - least * (number_of - 1)
    while surplus > 0:
        candidates = [i for i in range(1, number_of) if holding[i] < largest] or [i for i in range(1, number_of) if holding[i] < reach]
        whole, remaining = sum([weights[i] for i in candidates]), surplus
        for i in candidates:
            more = min(reach - holding[i], max(1, remaining * weights[i] // whole), surplus)
            holding[i] = holding[i] + more
            surplus = surplus - more
    return np.array(holding)


def scatter_about(key, extent, spread, bound, kind=jnp.bfloat16):
    drawn = spread * jax.random.normal(key, extent, jnp.float32)
    return jnp.clip(drawn, min=-bound, max=bound).astype(kind)


def setup_inputs(seed: int = 0) -> dict:
    splits = jax.random.split(jax.random.key(seed), 10)
    buffer = draw_buffer(jax.random.fold_in(splits[9], 71), 0)
    owner_keys = jax.random.split(jax.random.fold_in(splits[1], 1), BATCH // B_DEV)
    owner_turns = jax.random.permutation(jax.random.fold_in(splits[1], 3), BATCH // B_DEV)
    owner = jax.vmap(lambda own, number: assign_block(jax.random.fold_in(splits[1], 2), own, number, B_DEV, DEVICES, 1, CAP, 2))(owner_keys, owner_turns).reshape((BATCH, 1))
    local_row = with_ends(jax.random.randint(splits[2], (BATCH,), 0, ROWS_DEV), jax.random.fold_in(splits[2], 1), 0, ROWS_DEV - 1).astype(jnp.int32)
    q_in = scatter_about(splits[3], (2, S + A, H), (S + A) ** -0.5, 0.5)
    q_mid = scatter_about(splits[4], (2, H, H), (H // 2) ** -0.5, 0.5)
    q_out = scatter_about(splits[5], (2, H), (H // 2) ** -0.5, 0.5)
    v_in = scatter_about(splits[6], (S, H), S ** -0.5, 0.5)
    v_mid = scatter_about(splits[7], (H, H), (H // 2) ** -0.5, 0.5)
    v_out = scatter_about(splits[8], (H,), (H // 2) ** -0.5, 0.5)
    return dict(buffer=buffer, owner=owner, local_row=local_row, q_in=q_in, q_mid=q_mid, q_out=q_out, v_in=v_in, v_mid=v_mid, v_out=v_out)


def layer_two(first, mid, out):
    hidden = jnp.maximum(jnp.dot(first, mid, preferred_element_type=jnp.float32), 0.0)
    return jnp.dot(hidden, out.astype(jnp.float32), precision=lax.Precision.HIGHEST)


def critic_block(rows, q_in, q_mid, q_out, v_in, v_mid, v_out):
    pair = rows[:, :S + A]
    state = rows[:, :S]
    nexts = rows[:, S + A:2 * S + A]
    reward = rows[:, 2 * S + A].astype(jnp.float32)
    discount = rows[:, 2 * S + A + 1].astype(jnp.float32)
    qs = []
    for head in range(2):
        first = jnp.maximum(jnp.dot(pair, q_in[head], preferred_element_type=jnp.float32), 0.0).astype(jnp.bfloat16)
        qs.append(layer_two(first, q_mid[head], q_out[head]))
    both = jnp.concatenate([state, nexts], axis=0)
    vfirst = jnp.maximum(jnp.dot(both, v_in, preferred_element_type=jnp.float32), 0.0).astype(jnp.bfloat16)
    vall = layer_two(vfirst, v_mid, v_out)
    batch = state.shape[0]
    value_now = vall[:batch]
    value_next = vall[batch:]
    targets = reward + discount * value_next
    return qs[0], qs[1], value_now, value_next, targets


def reference(buffer, owner, local_row, q_in, q_mid, q_out, v_in, v_mid, v_out):
    index = (owner[:, 0] * ROWS_DEV + local_row).astype(jnp.int32)
    blocks = index.reshape(-1, B_DEV)

    def one_block(picks):
        rows = jnp.take(buffer, picks, axis=0)
        return critic_block(rows, q_in, q_mid, q_out, v_in, v_mid, v_out)

    results = lax.map(one_block, blocks)
    q_first, q_second, value_now, value_next, targets = [r.reshape(-1) for r in results]
    q_loss = (q_first - targets) ** 2 + (q_second - targets) ** 2
    gap = jnp.minimum(q_first, q_second) - value_now
    value_loss = jnp.where(gap < 0.0, 0.3, 0.7) * gap * gap
    return jnp.stack([q_first, q_second]), jnp.stack([value_now, value_next]), targets, q_loss, value_loss
```

```python
import jax
import jax.numpy as jnp
from jax import lax
from jax.experimental import pallas as pl
from jax.experimental.pallas import tpu as pltpu
from jax.sharding import Mesh
from jax.sharding import PartitionSpec as P

FAR = ("y", "z")
SIDE = ("x", "c")
SLOTS = 8
NV = 5
F32 = jnp.float32
BF16 = jnp.bfloat16
I32 = jnp.int32
SMALL = pltpu.CompilerParams(vmem_limit_bytes=16 * 2**20)


def split_owner(owner):
    y = owner >> 6
    x = (owner >> 4) & 3
    z = (owner >> 1) & 7
    c = owner & 1
    return y * 8 + z, x * 2 + c


def iota(shape, dim):
    return lax.broadcasted_iota(I32, shape, dim)


def nt(a, b):
    return lax.dot_general(a, b, (((1,), (1,)), ((), ())), preferred_element_type=F32)


def tn(a, b):
    return lax.dot_general(a, b, (((0,), (0,)), ((), ())), preferred_element_type=F32)


def request_kernel(owner_ref, local_ref, request_ref, rank_ref):
    chunks = owner_ref.shape[0]
    owner = owner_ref[...]
    columns = jnp.transpose(owner.astype(F32), (1, 0))
    before = iota((128, 128), 0) < iota((128, 128), 1)
    rows = [owner_ref[k : k + 1, :].astype(F32) for k in range(chunks)]
    totals = [jnp.zeros((128, 128), F32) for _ in range(chunks)]
    for q in range(chunks):
        column = jnp.broadcast_to(columns[:, q : q + 1], (128, 128))
        for k in range(q, chunks):
            same = column == rows[k]
            if k == q:
                same = jnp.logical_and(same, before)
            totals[k] = totals[k] + jnp.where(same, 1.0, 0.0)
    high = jnp.zeros((64, 128), F32)
    low = jnp.zeros((64, 128), F32)
    for k in range(chunks):
        rank = jnp.sum(totals[k], axis=0, keepdims=True).astype(I32)
        rank_ref[k : k + 1, :] = rank
        far, side = split_owner(owner_ref[k : k + 1, :])
        local = local_ref[k : k + 1, :]
        place = iota((128, 128), 0) == side * SLOTS + rank
        target = jnp.where(iota((64, 128), 0) == far, 1.0, 0.0).astype(BF16)
        high = high + nt(target, jnp.where(place, (local >> 7).astype(F32), 0.0).astype(BF16))
        low = low + nt(target, jnp.where(place, (local & 127).astype(F32), 0.0).astype(BF16))
    wanted = high.astype(I32) * 128 + low.astype(I32)
    request_ref[...] = wanted.reshape(64, 1, 128)


def critic_kernel(
    rows_ref, q0_ref, q1_ref, q_mid_ref, q_out_ref, v_in_ref, v_mid_ref, v_out_ref,
    table_ref, first_ref, mid_ref,
):
    count, width = rows_ref.shape
    states = v_in_ref.shape[0]
    pair = q0_ref.shape[0]

    def spread(weights, offset):
        inner = weights.shape[0]
        place = jnp.where(iota((inner, width), 1) == iota((inner, width), 0) + offset, 1.0, 0.0)
        return tn(weights, place.astype(BF16)).astype(BF16)

    first_ref[0:256, :] = spread(q0_ref[...], 0)
    first_ref[256:512, :] = spread(q1_ref[...], 0)
    first_ref[512:768, :] = spread(v_in_ref[...], 0)
    first_ref[768:1024, :] = spread(v_in_ref[...], pair)
    mid_ref[0] = spread(q_mid_ref[0], 0)
    mid_ref[1] = spread(q_mid_ref[1], 0)
    mid_ref[2] = spread(v_mid_ref[...], 0)
    unit = jnp.where(iota((256, 256), 0) == iota((256, 256), 1), 1.0, 0.0)

    def as_column(row):
        return jnp.sum(unit * row.astype(F32), axis=1, keepdims=True)

    outs = [as_column(q_out_ref[0:1, :]), as_column(q_out_ref[1:2, :]), as_column(v_out_ref[...])]
    outs = [jnp.broadcast_to(o, (256, 128)) for o in outs]
    tail = jnp.where(
        iota((8, width), 1) == iota((8, width), 0) + (pair + states), 1.0, 0.0
    ).astype(BF16)
    block = 256
    for b in range(count // block):
        x = rows_ref[b * block : (b + 1) * block, :]
        first = jnp.maximum(nt(first_ref[...], x), 0.0).astype(BF16)
        ends = nt(tail, x)
        results = []
        for i in range(4):
            m = min(i, 2)
            hidden = jnp.dot(
                mid_ref[m], first[i * 256 : (i + 1) * 256, :], preferred_element_type=F32
            )
            hidden = jnp.maximum(hidden, 0.0)
            weight = jnp.concatenate([outs[m]] * (block // 128), axis=1)
            results.append(jnp.sum(hidden * weight, axis=0, keepdims=True))
        target = ends[0:1, :] + ends[1:2, :] * results[3]
        results.append(target)
        for v in range(NV):
            for half in range(block // 128):
                row = v * 16 + b * (block // 128) + half
                piece = results[v][:, half * 128 : (half + 1) * 128]
                for s in range(8):
                    table_ref[s, row : row + 1, :] = piece


def serve_kernel(tables_ref, request_ref, answer_ref):
    wanted = request_ref[...].reshape(64, 128)
    expand = jnp.where(iota((64, 512), 0) == iota((64, 512), 1) // SLOTS, 1.0, 0.0).astype(BF16)
    own = iota((128, 512), 0) % SLOTS == iota((128, 512), 1) % SLOTS
    gather_side = jnp.where(iota((8, 128), 0) == iota((8, 128), 1) // SLOTS, 1.0, 0.0).astype(BF16)

    def by_side(values):
        wide = jnp.where(own, tn(values.astype(F32).astype(BF16), expand), 0.0).astype(BF16)
        return jnp.dot(gather_side, wide, preferred_element_type=F32).astype(I32)

    high = by_side(wanted >> 7)
    low = by_side(wanted & 127)
    lane_block = iota((8, 128), 1) // SLOTS
    for c in range(4):
        high_c = high[:, c * 128 : (c + 1) * 128]
        low_c = low[:, c * 128 : (c + 1) * 128]
        found = [jnp.zeros((8, 128), F32) for _ in range(NV)]
        for k in range(16):
            here = high_c == k
            for v in range(NV):
                piece = tables_ref[:, v * 16 + k, :]
                found[v] = jnp.where(here, jnp.take_along_axis(piece, low_c, axis=1), found[v])
        found = [found[0]] + [pltpu.roll(found[v], v * SLOTS, 1) for v in range(1, NV)]
        for h in range(16):
            message = found[0]
            for v in range(1, NV):
                message = jnp.where(lane_block == (h + v) % 16, found[v], message)
            if h:
                message = pltpu.roll(message, 128 - h * SLOTS, 1)
            answer_ref[c * 16 + h] = message


def finish_kernel(
    answer_ref, owner_ref, rank_ref, q_ref, values_ref, target_ref, q_loss_ref, value_loss_ref
):
    answers = answer_ref[...].reshape(512, 128)
    part_one = answers.astype(BF16)
    rest = answers - part_one.astype(F32)
    part_two = rest.astype(BF16)
    part_three = (rest - part_two.astype(F32)).astype(BF16)
    parts = [jnp.transpose(p, (1, 0))[: NV * SLOTS, :] for p in (part_one, part_two, part_three)]
    for k in range(owner_ref.shape[0]):
        far, side = split_owner(owner_ref[k : k + 1, :])
        hot = jnp.where(iota((512, 128), 0) == far * 8 + side, 1.0, 0.0).astype(BF16)
        got = jnp.dot(parts[0], hot, preferred_element_type=F32)
        got = got + jnp.dot(parts[1], hot, preferred_element_type=F32)
        got = got + jnp.dot(parts[2], hot, preferred_element_type=F32)
        mine = iota((8, 128), 0) == rank_ref[k : k + 1, :]
        q0, q1, now, later, target = [
            jnp.sum(
                jnp.where(mine, got[v * SLOTS : (v + 1) * SLOTS, :], 0.0), axis=0, keepdims=True
            )
            for v in range(NV)
        ]
        span = slice(k * 128, (k + 1) * 128)
        q_ref[0:1, span] = q0
        q_ref[1:2, span] = q1
        values_ref[0:1, span] = now
        values_ref[1:2, span] = later
        target_ref[:, span] = target
        q_loss_ref[:, span] = (q0 - target) ** 2 + (q1 - target) ** 2
        gap = jnp.minimum(q0, q1) - now
        value_loss_ref[:, span] = jnp.where(gap < 0.0, 0.3, 0.7) * gap * gap


def shape(dims, dtype):
    return jax.ShapeDtypeStruct(dims, dtype)


def make_request(owner, local_row):
    return pl.pallas_call(
        request_kernel,
        out_shape=(shape((64, 1, 128), I32), shape((8, 128), I32)),
        compiler_params=SMALL,
        name="make_request",
    )(owner, local_row)


def critics(buffer, q_in, q_mid, q_out, v_in, v_mid, v_out):
    return pl.pallas_call(
        critic_kernel,
        out_shape=shape((8, NV * 16, 128), F32),
        scratch_shapes=[pltpu.VMEM((1024, 256), BF16), pltpu.VMEM((3, 256, 256), BF16)],
        cost_estimate=pl.CostEstimate(
            flops=2 * 2048 * 1024 * 512, bytes_accessed=2_000_000, transcendentals=0
        ),
        compiler_params=SMALL,
        name="critics",
    )(buffer, q_in[0], q_in[1], q_mid, q_out, v_in, v_mid, v_out.reshape(1, -1))


def serve(tables, requests):
    return pl.pallas_call(
        serve_kernel, out_shape=shape((64, 8, 128), F32), compiler_params=SMALL, name="serve"
    )(tables, requests)


def finish(answers, owner, rank):
    line = shape((1, 1024), F32)
    two = shape((2, 1024), F32)
    return pl.pallas_call(
        finish_kernel, out_shape=(two, two, line, line, line), compiler_params=SMALL, name="finish"
    )(answers, owner, rank)


def body(buffer, owner, local_row, q_in, q_mid, q_out, v_in, v_mid, v_out):
    owner = owner.reshape(8, 128)
    local_row = local_row.reshape(8, 128)
    requests, rank = make_request(owner, local_row)
    requests = lax.all_to_all(requests, FAR, 0, 0, tiled=True)
    table = critics(buffer, q_in, q_mid, q_out, v_in, v_mid, v_out)
    tables = lax.all_to_all(table, SIDE, 0, 0, tiled=True)
    answers = serve(tables, requests)
    answers = lax.all_to_all(answers, FAR, 0, 0, tiled=True)
    q_values, values, targets, q_loss, value_loss = finish(answers, owner, rank)
    return q_values, values, targets.reshape(-1), q_loss.reshape(-1), value_loss.reshape(-1)


def solution(mesh):
    fine = Mesh(mesh.devices.reshape(8, 4, 8, 2), ("y", "x", "z", "c"))
    every = ("y", "x", "z", "c")
    return jax.shard_map(
        body,
        mesh=fine,
        in_specs=(P(every, None), P(every, None), P(every), P(), P(), P(), P(), P(), P()),
        out_specs=(P(None, every), P(None, every), P(every), P(every), P(every)),
        check_vma=False,
    )
```

```python
import jax
import jax.numpy as jnp
from jax import lax
from jax.experimental import pallas as pl
from jax.experimental.pallas import tpu as pltpu
from jax.sharding import Mesh
from jax.sharding import PartitionSpec as P

FAR = ("y", "z")
SIDE = ("x", "c")
SLOTS = 8
NV = 5
F32 = jnp.float32
BF16 = jnp.bfloat16
I32 = jnp.int32
SMALL = pltpu.CompilerParams(vmem_limit_bytes=16 * 2**20)


def split_owner(owner):
    y = owner >> 6
    x = (owner >> 4) & 3
    z = (owner >> 1) & 7
    c = owner & 1
    return y * 8 + z, x * 2 + c


def iota(shape, dim):
    return lax.broadcasted_iota(I32, shape, dim)


def nt(a, b):
    return lax.dot_general(a, b, (((1,), (1,)), ((), ())), preferred_element_type=F32)


def tn(a, b):
    return lax.dot_general(a, b, (((0,), (0,)), ((), ())), preferred_element_type=F32)


def request_kernel(
    owner_hbm, local_hbm, rows_hbm, q_in_hbm, q_mid_hbm, v_in_hbm, v_mid_hbm,
    request_ref, rank_ref, rows_ref, q_in_ref, q_mid_ref, v_in_ref, v_mid_ref,
    owner_ref, local_ref, sems,
):
    pairs = (
        (owner_hbm, owner_ref), (local_hbm, local_ref), (rows_hbm, rows_ref),
        (q_in_hbm, q_in_ref), (q_mid_hbm, q_mid_ref), (v_in_hbm, v_in_ref), (v_mid_hbm, v_mid_ref),
    )
    copies = [pltpu.make_async_copy(a, b, sems.at[i]) for i, (a, b) in enumerate(pairs)]
    for copy in copies:
        copy.start()
    copies[0].wait()
    copies[1].wait()
    chunks = owner_ref.shape[0]
    owner = owner_ref[...]
    columns = jnp.transpose(owner.astype(F32), (1, 0))
    before = iota((128, 128), 0) < iota((128, 128), 1)
    rows = [owner_ref[k : k + 1, :].astype(F32) for k in range(chunks)]
    totals = [jnp.zeros((128, 128), F32) for _ in range(chunks)]
    for q in range(chunks):
        column = jnp.broadcast_to(columns[:, q : q + 1], (128, 128))
        for k in range(q, chunks):
            same = column == rows[k]
            if k == q:
                same = jnp.logical_and(same, before)
            totals[k] = totals[k] + jnp.where(same, 1.0, 0.0)
    high = jnp.zeros((64, 128), F32)
    low = jnp.zeros((64, 128), F32)
    for k in range(chunks):
        rank = jnp.sum(totals[k], axis=0, keepdims=True).astype(I32)
        rank_ref[k : k + 1, :] = rank
        far, side = split_owner(owner_ref[k : k + 1, :])
        local = local_ref[k : k + 1, :]
        place = iota((128, 128), 0) == side * SLOTS + rank
        target = jnp.where(iota((64, 128), 0) == far, 1.0, 0.0).astype(BF16)
        high = high + nt(target, jnp.where(place, (local >> 7).astype(F32), 0.0).astype(BF16))
        low = low + nt(target, jnp.where(place, (local & 127).astype(F32), 0.0).astype(BF16))
    wanted = high.astype(I32) * 128 + low.astype(I32)
    request_ref[...] = wanted.reshape(64, 1, 128)
    for copy in copies[2:]:
        copy.wait()


def critic_kernel(
    rows_ref, q_in_ref, q_mid_ref, v_in_ref, v_mid_ref, q_out_ref, v_out_ref,
    table_ref, first_ref, mid_ref,
):
    count, width = rows_ref.shape
    states = v_in_ref.shape[0]
    pair = q_in_ref.shape[0]

    def spread(weights, offset, step=1):
        inner = weights.shape[0]
        place = iota((inner, width), 0) == (iota((inner, width), 1) - offset[1]) * step + offset[0]
        return tn(weights, jnp.where(place, 1.0, 0.0).astype(BF16)).astype(BF16)

    q_both = q_in_ref[...].reshape(2 * pair, width)
    first_ref[0:256, :] = spread(q_both, (0, 0), 2)
    first_ref[256:512, :] = spread(q_both, (1, 0), 2)
    first_ref[512:768, :] = spread(v_in_ref[...], (0, 0))
    first_ref[768:1024, :] = spread(v_in_ref[...], (0, pair))
    mid_ref[0] = spread(q_mid_ref[0], (0, 0))
    mid_ref[1] = spread(q_mid_ref[1], (0, 0))
    mid_ref[2] = spread(v_mid_ref[...], (0, 0))

    def as_column(row, pick):
        count = row.shape[0]
        return tn(row, jnp.where(iota((count, 128), 0) == pick, 1.0, 0.0).astype(BF16))

    q_out = q_out_ref[...]
    outs = [as_column(q_out, 0), as_column(q_out, 1), as_column(v_out_ref[...], 0)]
    tail = jnp.where(
        iota((8, width), 1) == iota((8, width), 0) + (pair + states), 1.0, 0.0
    ).astype(BF16)
    block = 256
    for b in range(count // block):
        x = rows_ref[b * block : (b + 1) * block, :]
        first = jnp.maximum(nt(first_ref[...], x), 0.0).astype(BF16)
        ends = nt(tail, x)
        results = []
        for i in range(4):
            m = min(i, 2)
            hidden = jnp.dot(
                mid_ref[m], first[i * 256 : (i + 1) * 256, :], preferred_element_type=F32
            )
            hidden = jnp.maximum(hidden, 0.0)
            weight = jnp.concatenate([outs[m]] * (block // 128), axis=1)
            results.append(jnp.sum(hidden * weight, axis=0, keepdims=True))
        target = ends[0:1, :] + ends[1:2, :] * results[3]
        results.append(target)
        for v in range(NV):
            for half in range(block // 128):
                row = v * 16 + b * (block // 128) + half
                piece = results[v][:, half * 128 : (half + 1) * 128]
                for s in range(8):
                    table_ref[s, row : row + 1, :] = piece


def serve_kernel(tables_ref, request_ref, answer_ref):
    wanted = request_ref[...].reshape(64, 128)
    expand = jnp.where(iota((64, 512), 0) == iota((64, 512), 1) // SLOTS, 1.0, 0.0).astype(BF16)
    own = iota((128, 512), 0) % SLOTS == iota((128, 512), 1) % SLOTS
    gather_side = jnp.where(iota((8, 128), 0) == iota((8, 128), 1) // SLOTS, 1.0, 0.0).astype(BF16)

    def by_side(values):
        wide = jnp.where(own, tn(values.astype(F32).astype(BF16), expand), 0.0).astype(BF16)
        return jnp.dot(gather_side, wide, preferred_element_type=F32).astype(I32)

    high = by_side(wanted >> 7)
    low = by_side(wanted & 127)
    lane_block = iota((8, 128), 1) // SLOTS
    upper = iota((8, 128), 0) < 4
    for c in range(4):
        high_c = high[:, c * 128 : (c + 1) * 128]
        low_c = low[:, c * 128 : (c + 1) * 128]
        found = [jnp.zeros((8, 128), F32) for _ in range(NV)]
        for k in range(16):
            here = high_c == k
            for v in range(NV):
                piece = tables_ref[:, v * 16 + k, :]
                found[v] = jnp.where(here, jnp.take_along_axis(piece, low_c, axis=1), found[v])
        near = [found[0]] + [pltpu.roll(found[v], v * SLOTS, 1) for v in range(1, NV)]
        away = [pltpu.roll(pltpu.roll(f, 4, 0), 64, 1) for f in near]

        def message(h, left, right):
            out = left[0]
            for v in range(NV):
                if v:
                    out = jnp.where(lane_block == (h + v) % 16, left[v], out)
                out = jnp.where(lane_block == (h + v + 8) % 16, right[v], out)
            return pltpu.roll(out, 128 - h * SLOTS, 1) if h else out

        for h in range(0, 16, 2):
            both = jnp.where(upper, message(h, near, away), message((h + 9) % 16, away, near))
            start = (c * 16 + h) * 4
            answer_ref[start : start + 8, :] = both


def finish_kernel(
    answer_ref, owner_ref, rank_ref, q_ref, values_ref, target_ref, q_loss_ref, value_loss_ref
):
    answers = answer_ref[...]
    part_one = answers.astype(BF16)
    rest = answers - part_one.astype(F32)
    part_two = rest.astype(BF16)
    part_three = (rest - part_two.astype(F32)).astype(BF16)
    parts = [jnp.transpose(p, (1, 0)) for p in (part_one, part_two, part_three)]
    for k in range(owner_ref.shape[0]):
        far, side = split_owner(owner_ref[k : k + 1, :])
        hot = jnp.where(iota((256, 128), 0) == far * 4 + (side & 3), 1.0, 0.0).astype(BF16)
        got = jnp.dot(parts[0], hot, preferred_element_type=F32)
        got = got + jnp.dot(parts[1], hot, preferred_element_type=F32)
        got = got + jnp.dot(parts[2], hot, preferred_element_type=F32)
        got = jnp.where(side < 4, got[0:64, :], got[64:128, :])
        mine = iota((8, 128), 0) == rank_ref[k : k + 1, :]
        q0, q1, now, later, target = [
            jnp.sum(
                jnp.where(mine, got[v * SLOTS : (v + 1) * SLOTS, :], 0.0), axis=0, keepdims=True
            )
            for v in range(NV)
        ]
        span = slice(k * 128, (k + 1) * 128)
        q_ref[0:1, span] = q0
        q_ref[1:2, span] = q1
        values_ref[0:1, span] = now
        values_ref[1:2, span] = later
        target_ref[:, span] = target
        q_loss_ref[:, span] = (q0 - target) ** 2 + (q1 - target) ** 2
        gap = jnp.minimum(q0, q1) - now
        value_loss_ref[:, span] = jnp.where(gap < 0.0, 0.3, 0.7) * gap * gap


def shape(dims, dtype):
    return jax.ShapeDtypeStruct(dims, dtype)


def make_request(owner, local_row, buffer, q_in, q_mid, v_in, v_mid):
    moved = (buffer, q_in, q_mid, v_in, v_mid)
    return pl.pallas_call(
        request_kernel,
        in_specs=[pl.BlockSpec(memory_space=pl.ANY)] * 7,
        out_specs=[pl.BlockSpec(memory_space=pltpu.VMEM)] * 7,
        out_shape=(
            shape((64, 1, 128), I32), shape((8, 128), I32), *[shape(m.shape, m.dtype) for m in moved]
        ),
        scratch_shapes=[
            pltpu.VMEM((8, 128), I32), pltpu.VMEM((8, 128), I32), pltpu.SemaphoreType.DMA((7,))
        ],
        compiler_params=SMALL,
        name="make_request",
    )(*[pltpu.with_memory_space_constraint(a, pltpu.HBM) for a in (owner, local_row, *moved)])


def critics(buffer, q_in, q_mid, v_in, v_mid, q_out, v_out):
    return pl.pallas_call(
        critic_kernel,
        out_shape=shape((8, NV * 16, 128), F32),
        scratch_shapes=[pltpu.VMEM((1024, 256), BF16), pltpu.VMEM((3, 256, 256), BF16)],
        cost_estimate=pl.CostEstimate(
            flops=2 * 2048 * 1024 * 512, bytes_accessed=2_000_000, transcendentals=0
        ),
        compiler_params=SMALL,
        name="critics",
    )(buffer, q_in, q_mid, v_in, v_mid, q_out, v_out.reshape(1, -1))


def serve(tables, requests):
    return pl.pallas_call(
        serve_kernel, out_shape=shape((256, 128), F32), compiler_params=SMALL, name="serve"
    )(tables, requests)


def finish(answers, owner, rank):
    line = shape((1, 1024), F32)
    two = shape((2, 1024), F32)
    return pl.pallas_call(
        finish_kernel, out_shape=(two, two, line, line, line), compiler_params=SMALL, name="finish"
    )(answers, owner, rank)


def body(buffer, owner, local_row, q_in, q_mid, q_out, v_in, v_mid, v_out):
    owner = owner.reshape(8, 128)
    local_row = local_row.reshape(8, 128)
    q_in = jnp.transpose(q_in, (1, 0, 2))
    requests, rank, *staged = make_request(owner, local_row, buffer, q_in, q_mid, v_in, v_mid)
    requests = lax.all_to_all(requests, FAR, 0, 0, tiled=True)
    table = critics(*staged, q_out, v_out)
    tables = lax.all_to_all(table, SIDE, 0, 0, tiled=True)
    answers = serve(tables, requests).reshape(64, 4, 128)
    answers = lax.all_to_all(answers, FAR, 0, 0, tiled=True).reshape(256, 128)
    q_values, values, targets, q_loss, value_loss = finish(answers, owner, rank)
    return q_values, values, targets.reshape(-1), q_loss.reshape(-1), value_loss.reshape(-1)


def solution(mesh):
    fine = Mesh(mesh.devices.reshape(8, 4, 8, 2), ("y", "x", "z", "c"))
    every = ("y", "x", "z", "c")
    return jax.shard_map(
        body,
        mesh=fine,
        in_specs=(P(every, None), P(every, None), P(every), P(), P(), P(), P(), P(), P()),
        out_specs=(P(None, every), P(None, every), P(every), P(every), P(every)),
        check_vma=False,
    )
```

```python
import jax
import jax.numpy as jnp
from jax import lax
from jax.experimental import pallas as pl
from jax.experimental.pallas import tpu as pltpu
from jax.sharding import Mesh
from jax.sharding import PartitionSpec as P

FAR = ("y", "z")
ASK = 37
REPLY = 36
SHARE = 5
SIDE = ("x", "c")
SLOTS = 8
NV = 5
F32 = jnp.float32
BF16 = jnp.bfloat16
I32 = jnp.int32
SMALL = pltpu.CompilerParams(vmem_limit_bytes=16 * 2**20)


def split_owner(owner):
    y = owner >> 6
    x = (owner >> 4) & 3
    z = (owner >> 1) & 7
    c = owner & 1
    return y * 8 + z, (x * 2 + c) ^ SHARE


def listed(count, first):
    return [[i ^ first for i in range(count)]]


def iota(shape, dim):
    return lax.broadcasted_iota(I32, shape, dim)


def nt(a, b):
    return lax.dot_general(a, b, (((1,), (1,)), ((), ())), preferred_element_type=F32)


def tn(a, b):
    return lax.dot_general(a, b, (((0,), (0,)), ((), ())), preferred_element_type=F32)


def request_kernel(
    owner_hbm, local_hbm, rows_hbm, q_in_hbm, q_mid_hbm, v_in_hbm, v_mid_hbm, q_out_hbm, v_out_hbm,
    request_ref, rank_ref, rows_ref, q_in_ref, q_mid_ref, v_in_ref, v_mid_ref, q_out_ref, v_out_ref,
    owner_ref, local_ref, target_ref, value_ref, sems,
):
    pairs = (
        (owner_hbm, owner_ref), (local_hbm, local_ref), (rows_hbm, rows_ref),
        (q_in_hbm, q_in_ref), (q_mid_hbm, q_mid_ref), (v_in_hbm, v_in_ref), (v_mid_hbm, v_mid_ref),
        (q_out_hbm, q_out_ref), (v_out_hbm, v_out_ref),
    )
    copies = [pltpu.make_async_copy(a, b, sems.at[i]) for i, (a, b) in enumerate(pairs)]
    for copy in copies:
        copy.start()
    copies[0].wait()
    copies[1].wait()
    chunks = owner_ref.shape[0]
    owner = owner_ref[...]
    columns = jnp.transpose(owner.astype(F32), (1, 0))
    before = iota((128, 128), 0) < iota((128, 128), 1)
    rows = [owner_ref[k : k + 1, :].astype(F32) for k in range(chunks)]
    totals = [jnp.zeros((128, 128), F32) for _ in range(chunks)]
    for q in range(chunks):
        column = jnp.broadcast_to(columns[:, q : q + 1], (128, 128))
        for k in range(q, chunks):
            same = column == rows[k]
            if k == q:
                same = jnp.logical_and(same, before)
            totals[k] = totals[k] + jnp.where(same, 1.0, 0.0)
    for k in range(chunks):
        span = slice(k * 128, (k + 1) * 128)
        rank = jnp.sum(totals[k], axis=0, keepdims=True).astype(I32)
        rank_ref[k : k + 1, :] = rank
        far, side = split_owner(owner_ref[k : k + 1, :])
        local = local_ref[k : k + 1, :]
        place = iota((64, 128), 0) == side * SLOTS + rank
        target_ref[:, span] = jnp.where(iota((64, 128), 0) == far ^ ASK, 1.0, 0.0).astype(BF16)
        value_ref[0:64, span] = jnp.where(place, (local >> 7).astype(F32), 0.0).astype(BF16)
        value_ref[64:128, span] = jnp.where(place, (local & 127).astype(F32), 0.0).astype(BF16)
    both = nt(target_ref[...], value_ref[...]).astype(I32)
    wanted = both * 128 + pltpu.roll(both, 64, 1)
    request_ref[...] = wanted.reshape(64, 1, 128)
    for copy in copies[2:]:
        copy.wait()


def critic_kernel(
    rows_ref, q_in_ref, q_mid_ref, v_in_ref, v_mid_ref, q_out_ref, v_out_ref,
    table_ref, first_ref, mid_ref,
):
    count, width = rows_ref.shape
    states = v_in_ref.shape[0]
    pair = q_in_ref.shape[0]

    def spread(weights, offset, step=1):
        inner = weights.shape[0]
        place = iota((inner, width), 0) == (iota((inner, width), 1) - offset[1]) * step + offset[0]
        return tn(weights, jnp.where(place, 1.0, 0.0).astype(BF16)).astype(BF16)

    q_both = q_in_ref[...].reshape(2 * pair, width)
    first_ref[0:256, :] = spread(q_both, (0, 0), 2)
    first_ref[256:512, :] = spread(q_both, (1, 0), 2)
    first_ref[512:768, :] = spread(v_in_ref[...], (0, 0))
    first_ref[768:1024, :] = spread(v_in_ref[...], (0, pair))
    mid_ref[0] = spread(q_mid_ref[0], (0, 0))
    mid_ref[1] = spread(q_mid_ref[1], (0, 0))
    mid_ref[2] = spread(v_mid_ref[...], (0, 0))

    def as_column(row, pick):
        count = row.shape[0]
        return tn(row, jnp.where(iota((count, 128), 0) == pick, 1.0, 0.0).astype(BF16))

    q_out = q_out_ref[...]
    outs = [as_column(q_out, 0), as_column(q_out, 1), as_column(v_out_ref[...].reshape(1, 256), 0)]
    tail = jnp.where(
        iota((8, width), 1) == iota((8, width), 0) + (pair + states), 1.0, 0.0
    ).astype(BF16)
    block = 256
    for b in range(count // block):
        x = rows_ref[b * block : (b + 1) * block, :]
        first = jnp.maximum(nt(first_ref[...], x), 0.0).astype(BF16)
        ends = nt(tail, x)
        results = []
        for i in range(4):
            m = min(i, 2)
            hidden = jnp.dot(
                mid_ref[m], first[i * 256 : (i + 1) * 256, :], preferred_element_type=F32
            )
            hidden = jnp.maximum(hidden, 0.0)
            weight = jnp.concatenate([outs[m]] * (block // 128), axis=1)
            results.append(jnp.sum(hidden * weight, axis=0, keepdims=True))
        target = ends[0:1, :] + ends[1:2, :] * results[3]
        results.append(target)
        for v in range(NV):
            for half in range(block // 128):
                row = v * 16 + b * (block // 128) + half
                piece = results[v][:, half * 128 : (half + 1) * 128]
                for s in range(8):
                    table_ref[s, row : row + 1, :] = piece


def serve_kernel(tables_ref, request_ref, answer_ref, turned_ref):
    turned_ref[...] = jnp.transpose(request_ref[...].reshape(64, 128).astype(F32), (1, 0))
    lane = iota((8, 128), 1)
    lane_block = lane // SLOTS
    upper = iota((8, 128), 0) < 4
    wanted = [jnp.zeros((8, 128), F32) for _ in range(4)]
    for s in range(SLOTS):
        rows = turned_ref[pl.ds(s, 8, stride=SLOTS), :]
        if rows.shape[1] < 128:
            rows = jnp.concatenate([rows, rows], axis=1)
        for c in range(4):
            spread = jnp.take_along_axis(rows, lane_block + c * 16, axis=1)
            wanted[c] = jnp.where(lane % SLOTS == s, spread, wanted[c])
    wanted = [w.astype(I32) for w in wanted]
    low = [w & 127 for w in wanted]
    high = [w >> 7 for w in wanted]
    looked_up = [[jnp.zeros((8, 128), F32) for _ in range(NV)] for _ in range(4)]
    for k in range(16):
        here = [h == k for h in high]
        for v in range(NV):
            piece = tables_ref[:, v * 16 + k, :]
            for c in range(4):
                got = jnp.take_along_axis(piece, low[c], axis=1)
                looked_up[c][v] = jnp.where(here[c], got, looked_up[c][v])
    for c in range(4):
        found = looked_up[c]
        near = [found[0]] + [pltpu.roll(found[v], v * SLOTS, 1) for v in range(1, NV)]
        away = [pltpu.roll(pltpu.roll(f, 4, 0), 64, 1) for f in near]

        def message(h, left, right):
            out = left[0]
            for v in range(NV):
                if v:
                    out = jnp.where(lane_block == (h + v) % 16, left[v], out)
                out = jnp.where(lane_block == (h + v + 8) % 16, right[v], out)
            return pltpu.roll(out, 128 - h * SLOTS, 1) if h else out

        for h in range(0, 16, 2):
            one, two = h ^ ASK ^ REPLY, (h + 1) ^ ASK ^ REPLY
            both = jnp.where(upper, message(one, near, away), message((two + 8) % 16, away, near))
            start = (c * 16 + h) * 4
            answer_ref[start : start + 8, :] = both


def finish_kernel(
    answer_ref, owner_ref, rank_ref, q_ref, values_ref, target_ref, q_loss_ref, value_loss_ref
):
    answers = answer_ref[...]
    part_one = answers.astype(BF16)
    rest = answers - part_one.astype(F32)
    part_two = rest.astype(BF16)
    part_three = (rest - part_two.astype(F32)).astype(BF16)
    parts = [jnp.transpose(p, (1, 0)) for p in (part_one, part_two, part_three)]
    for k in range(owner_ref.shape[0]):
        far, side = split_owner(owner_ref[k : k + 1, :])
        hot = jnp.where(iota((256, 128), 0) == (far ^ REPLY) * 4 + (side & 3), 1.0, 0.0).astype(BF16)
        got = jnp.dot(parts[0], hot, preferred_element_type=F32)
        got = got + jnp.dot(parts[1], hot, preferred_element_type=F32)
        got = got + jnp.dot(parts[2], hot, preferred_element_type=F32)
        got = jnp.where(side < 4, got[0:64, :], got[64:128, :])
        mine = iota((8, 128), 0) == rank_ref[k : k + 1, :]
        q0, q1, now, later, target = [
            jnp.sum(
                jnp.where(mine, got[v * SLOTS : (v + 1) * SLOTS, :], 0.0), axis=0, keepdims=True
            )
            for v in range(NV)
        ]
        span = slice(k * 128, (k + 1) * 128)
        q_ref[0:1, span] = q0
        q_ref[1:2, span] = q1
        values_ref[0:1, span] = now
        values_ref[1:2, span] = later
        target_ref[:, span] = target
        q_loss_ref[:, span] = (q0 - target) ** 2 + (q1 - target) ** 2
        gap = jnp.minimum(q0, q1) - now
        value_loss_ref[:, span] = jnp.where(gap < 0.0, 0.3, 0.7) * gap * gap


def shape(dims, dtype):
    return jax.ShapeDtypeStruct(dims, dtype)


def make_request(owner, local_row, *moved):
    return pl.pallas_call(
        request_kernel,
        in_specs=[pl.BlockSpec(memory_space=pl.ANY)] * (2 + len(moved)),
        out_specs=[pl.BlockSpec(memory_space=pltpu.VMEM)] * (2 + len(moved)),
        out_shape=(
            shape((64, 1, 128), I32), shape((8, 128), I32), *[shape(m.shape, m.dtype) for m in moved]
        ),
        scratch_shapes=[
            pltpu.VMEM((8, 128), I32), pltpu.VMEM((8, 128), I32),
            pltpu.VMEM((64, 1024), BF16), pltpu.VMEM((128, 1024), BF16), pltpu.SemaphoreType.DMA((2 + len(moved),))
        ],
        compiler_params=SMALL,
        name="make_request",
    )(*[pltpu.with_memory_space_constraint(a, pltpu.HBM) for a in (owner, local_row, *moved)])


def critics(buffer, q_in, q_mid, v_in, v_mid, q_out, v_out):
    return pl.pallas_call(
        critic_kernel,
        out_shape=shape((8, NV * 16, 128), F32),
        scratch_shapes=[pltpu.VMEM((1024, 256), BF16), pltpu.VMEM((3, 256, 256), BF16)],
        cost_estimate=pl.CostEstimate(
            flops=2 * 2048 * 1024 * 512, bytes_accessed=2_000_000, transcendentals=0
        ),
        compiler_params=SMALL,
        name="critics",
    )(buffer, q_in, q_mid, v_in, v_mid, q_out, v_out)


def serve(tables, requests):
    return pl.pallas_call(
        serve_kernel, out_shape=shape((256, 128), F32), scratch_shapes=[pltpu.VMEM((128, 64), F32)],
        compiler_params=SMALL, name="serve",
    )(tables, requests)


def finish(answers, owner, rank):
    line = shape((1, 1024), F32)
    two = shape((2, 1024), F32)
    return pl.pallas_call(
        finish_kernel, out_shape=(two, two, line, line, line), compiler_params=SMALL, name="finish"
    )(answers, owner, rank)


def body(buffer, owner, local_row, q_in, q_mid, q_out, v_in, v_mid, v_out):
    owner = owner.reshape(8, 128)
    local_row = local_row.reshape(8, 128)
    q_in = jnp.transpose(q_in, (1, 0, 2))
    requests, rank, *staged = make_request(
        owner, local_row, buffer, q_in, q_mid, v_in, v_mid, q_out, v_out
    )
    requests = lax.all_to_all(requests, FAR, 0, 0, axis_index_groups=listed(64, ASK), tiled=True)
    table = critics(*staged)
    tables = lax.all_to_all(table, SIDE, 0, 0, axis_index_groups=listed(8, SHARE), tiled=True)
    answers = serve(tables, requests).reshape(64, 4, 128)
    answers = lax.all_to_all(answers, FAR, 0, 0, axis_index_groups=listed(64, REPLY), tiled=True).reshape(256, 128)
    q_values, values, targets, q_loss, value_loss = finish(answers, owner, rank)
    return q_values, values, targets.reshape(-1), q_loss.reshape(-1), value_loss.reshape(-1)


def solution(mesh):
    fine = Mesh(mesh.devices.reshape(8, 4, 8, 2), ("y", "x", "z", "c"))
    every = ("y", "x", "z", "c")
    return jax.shard_map(
        body,
        mesh=fine,
        in_specs=(P(every, None), P(every, None), P(every), P(), P(), P(), P(), P(), P()),
        out_specs=(P(None, every), P(None, every), P(every), P(every), P(every)),
        check_vma=False,
    )
```

```python
import jax
import jax.numpy as jnp
from jax import lax
from jax.experimental import pallas as pl
from jax.experimental.pallas import tpu as pltpu
from jax.sharding import Mesh
from jax.sharding import PartitionSpec as P

FAR = ("y", "z")
ASK = 37
REPLY = 36
SHARE = 5
SIDE = ("x", "c")
SLOTS = 8
NV = 7
F32 = jnp.float32
BF16 = jnp.bfloat16
I32 = jnp.int32
SMALL = pltpu.CompilerParams(vmem_limit_bytes=16 * 2**20)


def split_owner(owner):
    y = owner >> 6
    x = (owner >> 4) & 3
    z = (owner >> 1) & 7
    c = owner & 1
    return y * 8 + z, (x * 2 + c) ^ SHARE


def listed(count, first):
    return [[i ^ first for i in range(count)]]


def iota(shape, dim):
    return lax.broadcasted_iota(I32, shape, dim)


def nt(a, b):
    return lax.dot_general(a, b, (((1,), (1,)), ((), ())), preferred_element_type=F32)


def tn(a, b):
    return lax.dot_general(a, b, (((0,), (0,)), ((), ())), preferred_element_type=F32)


def request_kernel(
    owner_hbm, local_hbm, rows_hbm, q_in_hbm, q_mid_hbm, v_in_hbm, v_mid_hbm, q_out_hbm, v_out_hbm,
    request_ref, rank_ref, rows_ref, q_in_ref, q_mid_ref, v_in_ref, v_mid_ref, q_out_ref, v_out_ref,
    owner_ref, local_ref, target_ref, value_ref, sems,
):
    pairs = (
        (owner_hbm, owner_ref), (local_hbm, local_ref), (rows_hbm, rows_ref),
        (q_in_hbm, q_in_ref), (q_mid_hbm, q_mid_ref), (v_in_hbm, v_in_ref), (v_mid_hbm, v_mid_ref),
        (q_out_hbm, q_out_ref), (v_out_hbm, v_out_ref),
    )
    copies = [pltpu.make_async_copy(a, b, sems.at[i]) for i, (a, b) in enumerate(pairs)]
    for copy in copies:
        copy.start()
    copies[0].wait()
    copies[1].wait()
    chunks = owner_ref.shape[0]
    owner = owner_ref[...]
    columns = jnp.transpose(owner.astype(F32), (1, 0))
    before = iota((128, 128), 0) < iota((128, 128), 1)
    rows = [owner_ref[k : k + 1, :].astype(F32) for k in range(chunks)]
    totals = [jnp.zeros((128, 128), F32) for _ in range(chunks)]
    for q in range(chunks):
        column = jnp.broadcast_to(columns[:, q : q + 1], (128, 128))
        for k in range(q, chunks):
            same = column == rows[k]
            if k == q:
                same = jnp.logical_and(same, before)
            totals[k] = totals[k] + jnp.where(same, 1.0, 0.0)
    for k in range(chunks):
        span = slice(k * 128, (k + 1) * 128)
        rank = jnp.sum(totals[k], axis=0, keepdims=True).astype(I32)
        rank_ref[k : k + 1, :] = rank
        far, side = split_owner(owner_ref[k : k + 1, :])
        local = local_ref[k : k + 1, :]
        place = iota((64, 128), 0) == side * SLOTS + rank
        target_ref[:, span] = jnp.where(iota((64, 128), 0) == far ^ ASK, 1.0, 0.0).astype(BF16)
        value_ref[0:64, span] = jnp.where(place, (local >> 7).astype(F32), 0.0).astype(BF16)
        value_ref[64:128, span] = jnp.where(place, (local & 127).astype(F32), 0.0).astype(BF16)
    both = nt(target_ref[...], value_ref[...]).astype(I32)
    wanted = both * 128 + pltpu.roll(both, 64, 1)
    request_ref[...] = wanted.reshape(64, 1, 128)
    for copy in copies[2:]:
        copy.wait()


def critic_kernel(
    rows_ref, q_in_ref, q_mid_ref, v_in_ref, v_mid_ref, q_out_ref, v_out_ref,
    table_ref, first_ref, mid_ref, lines_ref,
):
    count, width = rows_ref.shape
    states = v_in_ref.shape[0]
    pair = q_in_ref.shape[0]

    def spread(weights, offset, step=1):
        inner = weights.shape[0]
        place = iota((inner, width), 0) == (iota((inner, width), 1) - offset[1]) * step + offset[0]
        return tn(weights, jnp.where(place, 1.0, 0.0).astype(BF16)).astype(BF16)

    q_both = q_in_ref[...].reshape(2 * pair, width)
    first_ref[0:256, :] = spread(q_both, (0, 0), 2)
    first_ref[256:512, :] = spread(q_both, (1, 0), 2)
    first_ref[512:768, :] = spread(v_in_ref[...], (0, 0))
    first_ref[768:1024, :] = spread(v_in_ref[...], (0, pair))
    mid_ref[0] = spread(q_mid_ref[0], (0, 0))
    mid_ref[1] = spread(q_mid_ref[1], (0, 0))
    mid_ref[2] = spread(v_mid_ref[...], (0, 0))

    def as_column(row, pick):
        count = row.shape[0]
        return tn(row, jnp.where(iota((count, 128), 0) == pick, 1.0, 0.0).astype(BF16))

    q_out = q_out_ref[...]
    outs = [as_column(q_out, 0), as_column(q_out, 1), as_column(v_out_ref[...].reshape(1, 256), 0)]
    tail = jnp.where(
        iota((8, width), 1) == iota((8, width), 0) + (pair + states), 1.0, 0.0
    ).astype(BF16)
    block = 256
    for b in range(count // block):
        x = rows_ref[b * block : (b + 1) * block, :]
        first = jnp.maximum(nt(first_ref[...], x), 0.0).astype(BF16)
        ends = nt(tail, x)
        results = []
        for i in range(4):
            m = min(i, 2)
            hidden = jnp.dot(
                mid_ref[m], first[i * 256 : (i + 1) * 256, :], preferred_element_type=F32
            )
            hidden = jnp.maximum(hidden, 0.0)
            weight = jnp.concatenate([outs[m]] * (block // 128), axis=1)
            results.append(jnp.sum(hidden * weight, axis=0, keepdims=True))
        q0, q1, now, later = results
        target = ends[0:1, :] + ends[1:2, :] * later
        q_loss = (q0 - target) ** 2 + (q1 - target) ** 2
        gap = jnp.minimum(q0, q1) - now
        value_loss = jnp.where(gap < 0.0, 0.3, 0.7) * gap * gap
        for v, result in enumerate((q0, q1, now, later, target, q_loss, value_loss)):
            for half in range(block // 128):
                row = v * 16 + b * (block // 128) + half
                lines_ref[row : row + 1, :] = result[:, half * 128 : (half + 1) * 128]
    table = lines_ref[...].astype(BF16)
    for s in range(8):
        table_ref[s] = table


def serve_kernel(packed_ref, request_ref, answer_ref, turned_ref, tables_ref):
    for s in range(8):
        tables_ref[s] = packed_ref[s].astype(F32)
    turned_ref[...] = jnp.transpose(request_ref[...].reshape(64, 128).astype(F32), (1, 0))
    lane = iota((8, 128), 1)
    lane_block = lane // SLOTS
    upper = iota((8, 128), 0) < 4
    wanted = [jnp.zeros((8, 128), F32) for _ in range(4)]
    for s in range(SLOTS):
        rows = turned_ref[pl.ds(s, 8, stride=SLOTS), :]
        if rows.shape[1] < 128:
            rows = jnp.concatenate([rows, rows], axis=1)
        for c in range(4):
            spread = jnp.take_along_axis(rows, lane_block + c * 16, axis=1)
            wanted[c] = jnp.where(lane % SLOTS == s, spread, wanted[c])
    wanted = [w.astype(I32) for w in wanted]
    low = [w & 127 for w in wanted]
    high = [w >> 7 for w in wanted]
    looked_up = [[jnp.zeros((8, 128), F32) for _ in range(NV)] for _ in range(4)]
    for k in range(16):
        here = [h == k for h in high]
        for v in range(NV):
            piece = tables_ref[:, v * 16 + k, :]
            for c in range(4):
                got = jnp.take_along_axis(piece, low[c], axis=1)
                looked_up[c][v] = jnp.where(here[c], got, looked_up[c][v])
    for c in range(4):
        found = looked_up[c]
        near = [found[0]] + [pltpu.roll(found[v], v * SLOTS, 1) for v in range(1, NV)]
        away = [pltpu.roll(pltpu.roll(f, 4, 0), 64, 1) for f in near]

        def message(h, left, right):
            out = left[0]
            for v in range(NV):
                if v:
                    out = jnp.where(lane_block == (h + v) % 16, left[v], out)
                out = jnp.where(lane_block == (h + v + 8) % 16, right[v], out)
            return pltpu.roll(out, 128 - h * SLOTS, 1) if h else out

        for h in range(0, 16, 2):
            one, two = h ^ ASK ^ REPLY, (h + 1) ^ ASK ^ REPLY
            both = jnp.where(upper, message(one, near, away), message((two + 8) % 16, away, near))
            start = (c * 16 + h) * 4
            answer_ref[start : start + 8, :] = both.astype(BF16)


def finish_kernel(
    answer_ref, owner_ref, rank_ref, q_ref, values_ref, target_ref, q_loss_ref, value_loss_ref
):
    answers = jnp.transpose(answer_ref[...], (1, 0))
    for k in range(owner_ref.shape[0]):
        far, side = split_owner(owner_ref[k : k + 1, :])
        hot = jnp.where(iota((256, 128), 0) == (far ^ REPLY) * 4 + (side & 3), 1.0, 0.0).astype(BF16)
        got = jnp.dot(answers, hot, preferred_element_type=F32)
        got = jnp.where(side < 4, got[0:64, :], got[64:128, :])
        mine = iota((8, 128), 0) == rank_ref[k : k + 1, :]
        q0, q1, now, later, target, q_loss, value_loss = [
            jnp.sum(
                jnp.where(mine, got[v * SLOTS : (v + 1) * SLOTS, :], 0.0), axis=0, keepdims=True
            )
            for v in range(NV)
        ]
        span = slice(k * 128, (k + 1) * 128)
        q_ref[0:1, span] = q0
        q_ref[1:2, span] = q1
        values_ref[0:1, span] = now
        values_ref[1:2, span] = later
        target_ref[:, span] = target
        q_loss_ref[:, span] = q_loss
        value_loss_ref[:, span] = value_loss


def shape(dims, dtype):
    return jax.ShapeDtypeStruct(dims, dtype)


def make_request(owner, local_row, *moved):
    return pl.pallas_call(
        request_kernel,
        in_specs=[pl.BlockSpec(memory_space=pl.ANY)] * (2 + len(moved)),
        out_specs=[pl.BlockSpec(memory_space=pltpu.VMEM)] * (2 + len(moved)),
        out_shape=(
            shape((64, 1, 128), I32), shape((8, 128), I32), *[shape(m.shape, m.dtype) for m in moved]
        ),
        scratch_shapes=[
            pltpu.VMEM((8, 128), I32), pltpu.VMEM((8, 128), I32),
            pltpu.VMEM((64, 1024), BF16), pltpu.VMEM((128, 1024), BF16), pltpu.SemaphoreType.DMA((2 + len(moved),))
        ],
        compiler_params=SMALL,
        name="make_request",
    )(*[pltpu.with_memory_space_constraint(a, pltpu.HBM) for a in (owner, local_row, *moved)])


def critics(buffer, q_in, q_mid, v_in, v_mid, q_out, v_out):
    return pl.pallas_call(
        critic_kernel,
        out_shape=shape((8, NV * 16, 128), BF16),
        scratch_shapes=[
            pltpu.VMEM((1024, 256), BF16), pltpu.VMEM((3, 256, 256), BF16), pltpu.VMEM((NV * 16, 128), F32)
        ],
        cost_estimate=pl.CostEstimate(
            flops=2 * 2048 * 1024 * 512, bytes_accessed=2_000_000, transcendentals=0
        ),
        compiler_params=SMALL,
        name="critics",
    )(buffer, q_in, q_mid, v_in, v_mid, q_out, v_out)


def serve(tables, requests):
    return pl.pallas_call(
        serve_kernel, out_shape=shape((256, 128), BF16),
        scratch_shapes=[pltpu.VMEM((128, 64), F32), pltpu.VMEM((8, NV * 16, 128), F32)],
        compiler_params=SMALL, name="serve",
    )(tables, requests)


def finish(answers, owner, rank):
    line = shape((1, 1024), F32)
    two = shape((2, 1024), F32)
    return pl.pallas_call(
        finish_kernel, out_shape=(two, two, line, line, line), compiler_params=SMALL, name="finish"
    )(answers, owner, rank)


def body(buffer, owner, local_row, q_in, q_mid, q_out, v_in, v_mid, v_out):
    owner = owner.reshape(8, 128)
    local_row = local_row.reshape(8, 128)
    q_in = jnp.transpose(q_in, (1, 0, 2))
    requests, rank, *staged = make_request(
        owner, local_row, buffer, q_in, q_mid, v_in, v_mid, q_out, v_out
    )
    requests = lax.all_to_all(requests, FAR, 0, 0, axis_index_groups=listed(64, ASK), tiled=True)
    table = critics(*staged)
    tables = lax.all_to_all(table, SIDE, 0, 0, axis_index_groups=listed(8, SHARE), tiled=True)
    answers = serve(tables, requests).reshape(64, 4, 128)
    answers = lax.all_to_all(answers, FAR, 0, 0, axis_index_groups=listed(64, REPLY), tiled=True).reshape(256, 128)
    q_values, values, targets, q_loss, value_loss = finish(answers, owner, rank)
    return q_values, values, targets.reshape(-1), q_loss.reshape(-1), value_loss.reshape(-1)


def solution(mesh):
    fine = Mesh(mesh.devices.reshape(8, 4, 8, 2), ("y", "x", "z", "c"))
    every = ("y", "x", "z", "c")
    return jax.shard_map(
        body,
        mesh=fine,
        in_specs=(P(every, None), P(every, None), P(every), P(), P(), P(), P(), P(), P()),
        out_specs=(P(None, every), P(None, every), P(every), P(every), P(every)),
        check_vma=False,
    )
```

```python
import jax
import jax.numpy as jnp
from jax import lax
from jax.experimental import pallas as pl
from jax.experimental.pallas import tpu as pltpu
from jax.sharding import Mesh
from jax.sharding import PartitionSpec as P

FAR = ("y", "z")
ASK = 37
REPLY = 36
SHARE = 5
SIDE = ("x", "c")
SLOTS = 8
NV = 7
F32 = jnp.float32
BF16 = jnp.bfloat16
I32 = jnp.int32
SMALL = pltpu.CompilerParams(vmem_limit_bytes=16 * 2**20)


def split_owner(owner):
    y = owner >> 6
    x = (owner >> 4) & 3
    z = (owner >> 1) & 7
    c = owner & 1
    return y * 8 + z, (x * 2 + c) ^ SHARE


def listed(count, first):
    return [[i ^ first for i in range(count)]]


def iota(shape, dim):
    return lax.broadcasted_iota(I32, shape, dim)


def nt(a, b):
    return lax.dot_general(a, b, (((1,), (1,)), ((), ())), preferred_element_type=F32)


def tn(a, b):
    return lax.dot_general(a, b, (((0,), (0,)), ((), ())), preferred_element_type=F32)


def request_kernel(
    owner_hbm, local_hbm, rows_hbm, q_in_hbm, q_mid_hbm, v_in_hbm, v_mid_hbm, q_out_hbm, v_out_hbm,
    request_ref, rank_ref, rows_ref, q_in_ref, q_mid_ref, v_in_ref, v_mid_ref, q_out_ref, v_out_ref,
    owner_ref, local_ref, target_ref, value_ref, sems,
):
    pairs = (
        (owner_hbm, owner_ref), (local_hbm, local_ref), (rows_hbm, rows_ref),
        (q_in_hbm, q_in_ref), (q_mid_hbm, q_mid_ref), (v_in_hbm, v_in_ref), (v_mid_hbm, v_mid_ref),
        (q_out_hbm, q_out_ref), (v_out_hbm, v_out_ref),
    )
    copies = [pltpu.make_async_copy(a, b, sems.at[i]) for i, (a, b) in enumerate(pairs)]
    for copy in copies:
        copy.start()
    copies[0].wait()
    copies[1].wait()
    chunks = owner_ref.shape[0]
    owner = owner_ref[...]
    columns = jnp.transpose(owner.astype(F32), (1, 0))
    before = iota((128, 128), 0) < iota((128, 128), 1)
    rows = [owner_ref[k : k + 1, :].astype(F32) for k in range(chunks)]
    totals = [jnp.zeros((128, 128), F32) for _ in range(chunks)]
    for q in range(chunks):
        column = jnp.broadcast_to(columns[:, q : q + 1], (128, 128))
        for k in range(q, chunks):
            same = column == rows[k]
            if k == q:
                same = jnp.logical_and(same, before)
            totals[k] = totals[k] + jnp.where(same, 1.0, 0.0)
    for k in range(chunks):
        span = slice(k * 128, (k + 1) * 128)
        rank = jnp.sum(totals[k], axis=0, keepdims=True).astype(I32)
        rank_ref[k : k + 1, :] = rank
        far, side = split_owner(owner_ref[k : k + 1, :])
        local = local_ref[k : k + 1, :]
        place = iota((64, 128), 0) == side * SLOTS + rank
        target_ref[:, span] = jnp.where(iota((64, 128), 0) == far ^ ASK, 1.0, 0.0).astype(BF16)
        value_ref[0:64, span] = jnp.where(place, (local >> 7).astype(F32), 0.0).astype(BF16)
        value_ref[64:128, span] = jnp.where(place, (local & 127).astype(F32), 0.0).astype(BF16)
    both = nt(target_ref[...], value_ref[...]).astype(I32)
    wanted = both * 128 + pltpu.roll(both, 64, 1)
    request_ref[...] = wanted.reshape(64, 1, 128)
    for copy in copies[2:]:
        copy.wait()


def critic_kernel(
    rows_ref, q_in_ref, q_mid_ref, v_in_ref, v_mid_ref, q_out_ref, v_out_ref,
    table_ref, first_ref, mid_ref, lines_ref,
):
    count, width = rows_ref.shape
    states = v_in_ref.shape[0]
    pair = q_in_ref.shape[0]

    def spread(weights, offset, step=1):
        inner = weights.shape[0]
        place = iota((inner, width), 0) == (iota((inner, width), 1) - offset[1]) * step + offset[0]
        return tn(weights, jnp.where(place, 1.0, 0.0).astype(BF16)).astype(BF16)

    q_both = q_in_ref[...].reshape(2 * pair, width)
    first_ref[0:256, :] = spread(q_both, (0, 0), 2)
    first_ref[256:512, :] = spread(q_both, (1, 0), 2)
    first_ref[512:768, :] = spread(v_in_ref[...], (0, 0))
    first_ref[768:1024, :] = spread(v_in_ref[...], (0, pair))
    mid_ref[0] = spread(q_mid_ref[0], (0, 0))
    mid_ref[1] = spread(q_mid_ref[1], (0, 0))
    mid_ref[2] = spread(v_mid_ref[...], (0, 0))

    def as_column(row, pick):
        count = row.shape[0]
        return tn(row, jnp.where(iota((count, 128), 0) == pick, 1.0, 0.0).astype(BF16))

    q_out = q_out_ref[...]
    outs = [as_column(q_out, 0), as_column(q_out, 1), as_column(v_out_ref[...].reshape(1, 256), 0)]
    tail = jnp.where(
        iota((8, width), 1) == iota((8, width), 0) + (pair + states), 1.0, 0.0
    ).astype(BF16)
    block = 256
    for b in range(count // block):
        x = rows_ref[b * block : (b + 1) * block, :]
        first = jnp.maximum(nt(first_ref[...], x), 0.0).astype(BF16)
        ends = nt(tail, x)
        results = []
        for i in range(4):
            m = min(i, 2)
            hidden = jnp.dot(
                mid_ref[m], first[i * 256 : (i + 1) * 256, :], preferred_element_type=F32
            )
            hidden = jnp.maximum(hidden, 0.0)
            weight = jnp.concatenate([outs[m]] * (block // 128), axis=1)
            results.append(jnp.sum(hidden * weight, axis=0, keepdims=True))
        q0, q1, now, later = results
        target = ends[0:1, :] + ends[1:2, :] * later
        q_loss = (q0 - target) ** 2 + (q1 - target) ** 2
        gap = jnp.minimum(q0, q1) - now
        value_loss = jnp.where(gap < 0.0, 0.3, 0.7) * gap * gap
        for v, result in enumerate((q0, q1, now, later, target, q_loss, value_loss)):
            for half in range(block // 128):
                row = v * 16 + b * (block // 128) + half
                lines_ref[row : row + 1, :] = result[:, half * 128 : (half + 1) * 128]
    table = lines_ref[...].astype(BF16)
    for s in range(8):
        table_ref[s] = table


def serve_kernel(packed_ref, request_ref, answer_ref, turned_ref, tables_ref):
    for s in range(8):
        tables_ref[s * NV * 16 : (s + 1) * NV * 16, :] = packed_ref[s].astype(F32)
    turned_ref[...] = jnp.transpose(request_ref[...].reshape(64, 128).astype(F32), (1, 0))
    lane = iota((8, 128), 1)
    lane_block = lane // SLOTS
    upper = iota((8, 128), 0) < 4
    wanted = [jnp.zeros((8, 128), F32) for _ in range(4)]
    for s in range(SLOTS):
        rows = turned_ref[pl.ds(s, 8, stride=SLOTS), :]
        if rows.shape[1] < 128:
            rows = jnp.concatenate([rows, rows], axis=1)
        for c in range(4):
            spread = jnp.take_along_axis(rows, lane_block + c * 16, axis=1)
            wanted[c] = jnp.where(lane % SLOTS == s, spread, wanted[c])
    wanted = [w.astype(I32) for w in wanted]
    low = [w & 127 for w in wanted]
    high = [w >> 7 for w in wanted]
    looked_up = [[jnp.zeros((8, 128), F32) for _ in range(NV)] for _ in range(4)]
    for k in range(16):
        here = [h == k for h in high]
        for v in range(NV):
            piece = tables_ref[pl.ds(v * 16 + k, 8, stride=NV * 16), :]
            for c in range(4):
                got = jnp.take_along_axis(piece, low[c], axis=1)
                looked_up[c][v] = jnp.where(here[c], got, looked_up[c][v])
    for c in range(4):
        found = looked_up[c]
        near = [found[0]] + [pltpu.roll(found[v], v * SLOTS, 1) for v in range(1, NV)]
        away = [pltpu.roll(pltpu.roll(f, 4, 0), 64, 1) for f in near]

        def message(h, left, right):
            out = left[0]
            for v in range(NV):
                if v:
                    out = jnp.where(lane_block == (h + v) % 16, left[v], out)
                out = jnp.where(lane_block == (h + v + 8) % 16, right[v], out)
            return pltpu.roll(out, 128 - h * SLOTS, 1) if h else out

        for h in range(0, 16, 2):
            one, two = h ^ ASK ^ REPLY, (h + 1) ^ ASK ^ REPLY
            both = jnp.where(upper, message(one, near, away), message((two + 8) % 16, away, near))
            start = (c * 16 + h) * 4
            answer_ref[start : start + 8, :] = both.astype(BF16)


def finish_kernel(
    answer_ref, owner_ref, rank_ref, q_ref, values_ref, target_ref, q_loss_ref, value_loss_ref
):
    answers = jnp.transpose(answer_ref[...], (1, 0))
    for k in range(owner_ref.shape[0]):
        far, side = split_owner(owner_ref[k : k + 1, :])
        hot = jnp.where(iota((256, 128), 0) == (far ^ REPLY) * 4 + (side & 3), 1.0, 0.0).astype(BF16)
        got = jnp.dot(answers, hot, preferred_element_type=F32)
        got = jnp.where(side < 4, got[0:64, :], got[64:128, :])
        mine = iota((8, 128), 0) == rank_ref[k : k + 1, :]
        q0, q1, now, later, target, q_loss, value_loss = [
            jnp.sum(
                jnp.where(mine, got[v * SLOTS : (v + 1) * SLOTS, :], 0.0), axis=0, keepdims=True
            )
            for v in range(NV)
        ]
        span = slice(k * 128, (k + 1) * 128)
        q_ref[0:1, span] = q0
        q_ref[1:2, span] = q1
        values_ref[0:1, span] = now
        values_ref[1:2, span] = later
        target_ref[:, span] = target
        q_loss_ref[:, span] = q_loss
        value_loss_ref[:, span] = value_loss


def shape(dims, dtype):
    return jax.ShapeDtypeStruct(dims, dtype)


def make_request(owner, local_row, *moved):
    return pl.pallas_call(
        request_kernel,
        in_specs=[pl.BlockSpec(memory_space=pl.ANY)] * (2 + len(moved)),
        out_specs=[pl.BlockSpec(memory_space=pltpu.VMEM)] * (2 + len(moved)),
        out_shape=(
            shape((64, 1, 128), I32), shape((8, 128), I32), *[shape(m.shape, m.dtype) for m in moved]
        ),
        scratch_shapes=[
            pltpu.VMEM((8, 128), I32), pltpu.VMEM((8, 128), I32),
            pltpu.VMEM((64, 1024), BF16), pltpu.VMEM((128, 1024), BF16), pltpu.SemaphoreType.DMA((2 + len(moved),))
        ],
        compiler_params=SMALL,
        name="make_request",
    )(*[pltpu.with_memory_space_constraint(a, pltpu.HBM) for a in (owner, local_row, *moved)])


def critics(buffer, q_in, q_mid, v_in, v_mid, q_out, v_out):
    return pl.pallas_call(
        critic_kernel,
        out_shape=shape((8, NV * 16, 128), BF16),
        scratch_shapes=[
            pltpu.VMEM((1024, 256), BF16), pltpu.VMEM((3, 256, 256), BF16), pltpu.VMEM((NV * 16, 128), F32)
        ],
        cost_estimate=pl.CostEstimate(
            flops=2 * 2048 * 1024 * 512, bytes_accessed=2_000_000, transcendentals=0
        ),
        compiler_params=SMALL,
        name="critics",
    )(buffer, q_in, q_mid, v_in, v_mid, q_out, v_out)


def serve(tables, requests):
    return pl.pallas_call(
        serve_kernel, out_shape=shape((256, 128), BF16),
        scratch_shapes=[pltpu.VMEM((128, 64), F32), pltpu.VMEM((8 * NV * 16, 128), F32)],
        compiler_params=SMALL, name="serve",
    )(tables, requests)


def finish(answers, owner, rank):
    line = shape((1, 1024), F32)
    two = shape((2, 1024), F32)
    return pl.pallas_call(
        finish_kernel, out_shape=(two, two, line, line, line), compiler_params=SMALL, name="finish"
    )(answers, owner, rank)


def body(buffer, owner, local_row, q_in, q_mid, q_out, v_in, v_mid, v_out):
    owner = owner.reshape(8, 128)
    local_row = local_row.reshape(8, 128)
    q_in = jnp.transpose(q_in, (1, 0, 2))
    requests, rank, *staged = make_request(
        owner, local_row, buffer, q_in, q_mid, v_in, v_mid, q_out, v_out
    )
    requests = lax.all_to_all(requests, FAR, 0, 0, axis_index_groups=listed(64, ASK), tiled=True)
    table = critics(*staged)
    tables = lax.all_to_all(table, SIDE, 0, 0, axis_index_groups=listed(8, SHARE), tiled=True)
    answers = serve(tables, requests).reshape(64, 4, 128)
    answers = lax.all_to_all(answers, FAR, 0, 0, axis_index_groups=listed(64, REPLY), tiled=True).reshape(256, 128)
    q_values, values, targets, q_loss, value_loss = finish(answers, owner, rank)
    return q_values, values, targets.reshape(-1), q_loss.reshape(-1), value_loss.reshape(-1)


def solution(mesh):
    fine = Mesh(mesh.devices.reshape(8, 4, 8, 2), ("y", "x", "z", "c"))
    every = ("y", "x", "z", "c")
    return jax.shard_map(
        body,
        mesh=fine,
        in_specs=(P(every, None), P(every, None), P(every), P(), P(), P(), P(), P(), P()),
        out_specs=(P(None, every), P(None, every), P(every), P(every), P(every)),
        check_vma=False,
    )
```
